32 devices in a mesh: groups: 2 (over y), grid: 16 (over z, x, core).
Axes of the slice: x: 2, y: 2, z: 4, core: 2. Of those that a mesh axis runs over, the one named last changes fastest.
Arguments:
- start_field: float32 [32, 1024, 128], P(('groups', 'grid')), parts along dimension 0, may hold values from -6 to 6
- col_speed: float32 [1024], replicated, may hold values from 0.5 to 2
- row_speed: float32 [32], replicated, may hold values from 0.5 to 2
- levels: int32 [32], P('groups'), parts along dimension 0, may hold values from 2 to 5, as said below
- coeffs: int32 [32], P('groups'), parts along dimension 0, may hold values from 1 to 3
- assign_first: int32 [32], P('groups'), parts along dimension 0, may hold values from 0 to 15, each once
- assign_second: int32 [32], P('groups'), parts along dimension 0, may hold values from 0 to 15, each once
- owner_of: int32 [32], P('groups'), parts along dimension 0, may hold values from 0 to 15, each once
Outputs:
- combined: float32 [2048, 1280], P(('groups', 'grid')), parts along dimension 0
- final_field: float32 [32, 1024, 128], P(('groups', 'grid')), parts along dimension 0
The draws below stay inside these ranges and needn't reach their ends.
There are 2 independent parts, one for each index of `groups`. The reference program is written for one: setup_inputs(seed, part) draws one part's arguments, and reference() takes and returns one part's arrays. A program takes and returns all parts, laid end to end along the dimension named above; an argument that names none is the same for every part. Nothing has to cross between parts.
Inputs may be any that keep to these rules, and one draw needn't show every extreme that they name: `levels`: every run of 4 consecutive grids starting at a multiple of 4 holds each first level from 2 to 5 exactly once.
All inputs are finite; a program needn't handle non-finite values.
Results may differ from the reference program's by a relative error of at most 0.0003.
Values sent between devices are 32-bit elements; how exact they have to be, the bound alone decides.
No kernel may reach another device: no remote copies, remote signals or barrier semaphores. Data moves between devices by JAX's collectives and lax.ppermute only.
A program may use at most 64 MiB of HBM per device.

```python
import math
import jax
import jax.numpy as jnp
import numpy as np
from jax import lax

LMIN = 2
NLEV = 4
CLEV = 5
STEPS = 2
ROWS = 128
COLS = 1024
CROWS = 320
FINE = 32
NGRID = 16
NPOS = 4
BLOCK_COLS = 64
N_GRID = 16


def draw_levels(key, part):
    rows_of = NGRID // NLEV
    scores = jax.random.randint(key, (rows_of, NLEV), 0, 1 << 20)
    scores = scores * NLEV + jnp.arange(NLEV, dtype=jnp.int32)[None, :]
    order_of = jnp.argsort(scores, axis=1)
    return (LMIN + order_of).reshape(NGRID).astype(jnp.int32)


def with_ends(drawn, rng, least, high):
    shape = drawn.shape
    index_at = [jax.random.randint(jax.random.fold_in(rng, axis), (), 0, shape[axis]) for axis in range(len(shape))]
    drawn = drawn.at[tuple(index_at)].set(least)
    longest = shape.index(max(shape))
    index_at[longest] = (index_at[longest] + 1) % shape[longest]
    return drawn.at[tuple(index_at)].set(high)


def steps_of(stream_key, dims, pieces, low, top_value):
    def one(axis_at, parts):
        draws = jax.random.uniform(jax.random.fold_in(jax.random.fold_in(stream_key, 6), axis_at), (parts,), jnp.float32, low / len(pieces), top_value / len(pieces))
        return jnp.repeat(jnp.exp(draws), dims[axis_at] // parts).reshape((-1,) + (1,) * (len(dims) - axis_at - 1))

    level = one(*pieces[0])
    for cut in pieces[1:]:
        level = level * one(*cut)
    return level


def normal_values(stream_key, extent, deviation, most, pieces=(), held_as=jnp.bfloat16):
    drawn = jax.random.normal(stream_key, extent, jnp.float32) * deviation
    if len(pieces) > 0:
        drawn = steps_of(stream_key, extent, pieces, -0.22, 0.18) * drawn
    return jnp.clip(drawn, min=-most, max=most).astype(held_as)


def setup_inputs(seed: int = 0, part: int = 0) -> dict:
    keys = jax.random.split(jax.random.key(seed), 9)
    own_keys = jax.random.split(jax.random.fold_in(keys[8], part), 9)
    start_field = normal_values(own_keys[0], (N_GRID, COLS, ROWS), 1.0, 6.0, ((0, 16),), jnp.float32)
    col_speed = jnp.clip(jnp.exp(jax.random.uniform(keys[1], (COLS,), jnp.float32, math.log(0.5), math.log(2.0))), 0.5, 2.0)
    row_speed = jnp.clip(jnp.exp(jax.random.uniform(keys[2], (FINE,), jnp.float32, math.log(0.5), math.log(2.0))), 0.5, 2.0)
    levels = draw_levels(jax.random.fold_in(jax.random.fold_in(keys[8], part), 71), part)
    coeffs = with_ends(jax.random.randint(own_keys[4], (NGRID,), 1, 4), jax.random.fold_in(own_keys[4], 1), 1, 3).astype(jnp.int32)
    assign_first = jax.random.permutation(own_keys[5], NGRID).astype(jnp.int32)
    assign_second = jax.random.permutation(own_keys[6], NGRID).astype(jnp.int32)
    owner_of = jax.random.permutation(own_keys[7], N_GRID).astype(jnp.int32)
    return {"start_field": start_field, "col_speed": col_speed, "row_speed": row_speed, "levels": levels, "coeffs": coeffs, "assign_first": assign_first, "assign_second": assign_second, "owner_of": owner_of}


time_step = 0.02
diffusivity = 0.0024
highest = lax.Precision.HIGHEST


def hier_line(line_level):
    points = 2 ** line_level
    matrix = np.zeros((points, points))
    matrix[0, 0] = 1.0
    for tier_rank in range(1, line_level + 1):
        stride = 2 ** (line_level - tier_rank)
        for entry_at in range(2 ** (tier_rank - 1), 2 ** tier_rank):
            node_at = (2 * (entry_at - 2 ** (tier_rank - 1)) + 1) * stride
            matrix[entry_at, node_at] += 1.0
            matrix[entry_at, (node_at - stride) % points] -= 0.5
            matrix[entry_at, (node_at + stride) % points] -= 0.5
    return matrix


def dehier_line(line_level):
    points = 2 ** line_level
    matrix = np.zeros((points, points))
    matrix[0, 0] = 1.0
    for tier_rank in range(1, line_level + 1):
        stride = 2 ** (line_level - tier_rank)
        for entry_at in range(2 ** (tier_rank - 1), 2 ** tier_rank):
            node_at = (2 * (entry_at - 2 ** (tier_rank - 1)) + 1) * stride
            matrix[node_at] = 0.5 * (matrix[(node_at - stride) % points] + matrix[(node_at + stride) % points])
            matrix[node_at, entry_at] += 1.0
    return matrix


def row_tables():
    row_bits = 2 * LMIN + NLEV - 1
    starts, widths, offsets = [], [], []
    running = 0
    for piece_level in range(LMIN, LMIN + NLEV):
        first_row = 0 if piece_level == LMIN else 2 ** (piece_level - 1)
        breadth = 2 ** LMIN if piece_level == LMIN else 2 ** (piece_level - 1)
        starts.append(first_row)
        widths.append(breadth)
        offsets.append(running)
        running += breadth * 2 ** (row_bits - piece_level)
    forward, backward, embeds, places = [], [], [], []
    for shift_level in range(NLEV):
        first_level = LMIN + shift_level
        second_level = row_bits - first_level
        tensor = np.kron(hier_line(first_level), hier_line(second_level))
        inverse = np.kron(dehier_line(first_level), dehier_line(second_level))
        order_list, place_list = [], []
        for slot_index in range(shift_level + 1):
            for second in range(2 ** second_level):
                for first_idx in range(starts[slot_index], starts[slot_index] + widths[slot_index]):
                    order_list.append(first_idx * 2 ** second_level + second)
                    place_list.append(offsets[slot_index] + second * widths[slot_index] + first_idx - starts[slot_index])
        embedding = np.zeros((running, 2 ** row_bits))
        embedding[np.array(place_list), np.arange(2 ** row_bits)] = 1.0
        forward.append(tensor[order_list])
        backward.append(inverse[:, order_list])
        embeds.append(embedding)
        places.append(place_list)
    return (jnp.asarray(np.stack(forward), jnp.float32), jnp.asarray(np.stack(backward), jnp.float32),
            jnp.asarray(np.stack(embeds), jnp.float32), jnp.asarray(np.array(places), jnp.int32))


def column_pass(values, matrix):
    side_cells = matrix.shape[0]
    cube_view = values.reshape(side_cells, side_cells, values.shape[-1])
    cube_view = jnp.einsum('ab,bjr->ajr', matrix, cube_view, precision=highest)
    cube_view = jnp.einsum('ab,jbr->jar', matrix, cube_view, precision=highest)
    return cube_view.reshape(values.shape)


def advance(values, grid_level, count, col_speed, row_speed):
    side_cells = 2 ** CLEV
    total_rows = values.shape[1]
    row_bits = 2 * LMIN + NLEV - 1
    other_level = row_bits - grid_level
    inner_count = jnp.left_shift(jnp.int32(1), other_level)
    inner_pos = jnp.bitwise_and(jnp.arange(total_rows, dtype=jnp.int32), inner_count - 1)
    sample_at = inner_pos * jnp.left_shift(jnp.int32(1), row_bits - LMIN - other_level)
    fine_cells = row_speed.shape[0]
    row_factor = jnp.sum(jnp.where(sample_at[:, None] == jnp.arange(fine_cells, dtype=jnp.int32)[None, :],
                                   row_speed[None, :], jnp.zeros_like(row_speed)[None, :]), axis=1)
    velocity = col_speed[:, None] * row_factor[None, :]
    refine = jnp.left_shift(jnp.int32(1), grid_level - LMIN)
    dt_sub = time_step / refine.astype(jnp.float32)
    scale_one = jnp.left_shift(jnp.int32(1), grid_level).astype(jnp.float32)
    scale_two = inner_count.astype(jnp.float32)
    coeff_side = float(4 ** CLEV)
    at_last = (inner_pos == inner_count - 1)[None, :]
    at_first = (inner_pos == 0)[None, :]

    def one_substep(turn_index, current):
        up_one = jnp.roll(current, -inner_count, axis=1)
        down_one = jnp.roll(current, inner_count, axis=1)
        up_two = jnp.where(at_last, jnp.roll(current, inner_count - 1, axis=1), jnp.roll(current, -1, axis=1))
        down_two = jnp.where(at_first, jnp.roll(current, 1 - inner_count, axis=1), jnp.roll(current, 1, axis=1))
        cube_view = current.reshape(side_cells, side_cells, total_rows)
        across = (jnp.roll(cube_view, 1, axis=0) + jnp.roll(cube_view, -1, axis=0)
                  + jnp.roll(cube_view, 1, axis=1) + jnp.roll(cube_view, -1, axis=1))
        across = across.reshape(current.shape) - 4.0 * current
        spread = (scale_one * scale_one * (up_one + down_one - 2.0 * current)
                  + scale_two * scale_two * (up_two + down_two - 2.0 * current) + coeff_side * across)
        transport = velocity * (up_one - down_one) * (0.5 * scale_one)
        return current + dt_sub * (diffusivity * spread - transport)

    return lax.fori_loop(jnp.int32(0), refine * count, one_substep, values)


def reference(start_field, col_speed, row_speed, levels, coeffs, assign_first, assign_second, owner_of):
    forward, backward, embeds, places = row_tables()
    column_hier = jnp.asarray(hier_line(CLEV), jnp.float32)
    column_back = jnp.asarray(dehier_line(CLEV), jnp.float32)
    cover = jnp.sum(embeds, axis=2)
    grid_ids = jnp.arange(NGRID, dtype=jnp.int32)
    weights = coeffs.astype(jnp.float32)
    denominator = (weights[:, None] * cover[levels - LMIN]).reshape(NPOS, NLEV, CROWS).sum(axis=1)

    def hier_one(inputs):
        values, grid_level = inputs
        mixed = column_pass(values, column_hier)
        return jnp.dot(mixed, forward[grid_level - LMIN].T, precision=highest)

    def dehier_one(values, grid_level):
        mixed = jnp.dot(values, backward[grid_level - LMIN].T, precision=highest)
        return column_pass(mixed, column_back)

    def combine(surplus):
        def spread_one(inputs):
            values, grid_level, weight = inputs
            return jnp.dot(values * weight, embeds[grid_level - LMIN].T, precision=highest)
        placed = lax.map(spread_one, (surplus, levels, weights))
        total = placed.reshape(NPOS, NLEV, COLS, CROWS).sum(axis=1)
        return total / denominator[:, None, :]

    def restrict(section_values):
        def take_one(inputs):
            grid_id, grid_level = inputs
            return jnp.dot(section_values[grid_id // NLEV], embeds[grid_level - LMIN], precision=highest)
        return lax.map(take_one, (grid_ids, levels))

    def first_cycle(inputs):
        values, grid_level = inputs
        return advance(values, grid_level, STEPS, col_speed, row_speed)

    def later_cycle(inputs):
        values, grid_level = inputs
        return advance(dehier_one(values, grid_level), grid_level, STEPS, col_speed, row_speed)

    def last_step(inputs):
        values, grid_level = inputs
        return advance(dehier_one(values, grid_level), grid_level, 1, col_speed, row_speed)

    current = lax.map(first_cycle, (start_field[assign_first], levels))
    first_combined = combine(lax.map(hier_one, (current, levels)))
    current = lax.map(later_cycle, (restrict(first_combined), levels))
    second_combined = combine(lax.map(hier_one, (current, levels)))
    current = lax.map(last_step, (restrict(second_combined), levels))
    final_field = jnp.zeros_like(current).at[assign_second].set(current)
    owner_ids = jnp.arange(N_GRID, dtype=jnp.int32)
    owner_inv = jnp.sum(jnp.where(owner_of[None, :] == owner_ids[:, None], owner_ids[None, :], 0), axis=1)
    blocks = jnp.transpose(second_combined, (1, 0, 2)).reshape(N_GRID, BLOCK_COLS, NPOS * CROWS)
    combined = blocks[owner_inv].reshape(COLS, NPOS * CROWS)
    return combined, final_field
```

```python
import functools

import jax
import jax.numpy as jnp
import numpy as np
from jax import lax
from jax.experimental import pallas as pl
from jax.experimental.pallas import tpu as pltpu
from jax.sharding import PartitionSpec as P

LMIN = 2
NLEV = 4
CLEV = 5
STEPS = 2

time_step = 0.02
diffusivity = 0.0024

SIDE = 2**CLEV
QUADS = SIDE // 8
ROW_BITS = 2 * LMIN + NLEV - 1
SHARED = 96
SMEM = pl.BlockSpec(memory_space=pltpu.SMEM)
VMEM = pl.BlockSpec(memory_space=pltpu.VMEM)


def hier_line(line_level):
    points = 2**line_level
    matrix = np.zeros((points, points))
    matrix[0, 0] = 1.0
    for tier_rank in range(1, line_level + 1):
        stride = 2 ** (line_level - tier_rank)
        for entry_at in range(2 ** (tier_rank - 1), 2**tier_rank):
            node_at = (2 * (entry_at - 2 ** (tier_rank - 1)) + 1) * stride
            matrix[entry_at, node_at] += 1.0
            matrix[entry_at, (node_at - stride) % points] -= 0.5
            matrix[entry_at, (node_at + stride) % points] -= 0.5
    return matrix


def dehier_line(line_level):
    points = 2**line_level
    matrix = np.zeros((points, points))
    matrix[0, 0] = 1.0
    for tier_rank in range(1, line_level + 1):
        stride = 2 ** (line_level - tier_rank)
        for entry_at in range(2 ** (tier_rank - 1), 2**tier_rank):
            node_at = (2 * (entry_at - 2 ** (tier_rank - 1)) + 1) * stride
            matrix[node_at] = 0.5 * (
                matrix[(node_at - stride) % points] + matrix[(node_at + stride) % points]
            )
            matrix[node_at, entry_at] += 1.0
    return matrix


def row_tables():
    starts = [0 if k == 0 else 2 ** (LMIN + k - 1) for k in range(NLEV)]
    widths = [2**LMIN if k == 0 else 2 ** (LMIN + k - 1) for k in range(NLEV)]
    forward, backward = ([], [])
    for shift_level in range(NLEV):
        first_level = LMIN + shift_level
        second_level = ROW_BITS - first_level
        tensor = np.kron(hier_line(first_level), hier_line(second_level))
        inverse = np.kron(dehier_line(first_level), dehier_line(second_level))
        order_list = []
        for slot_index in range(shift_level + 1):
            for second in range(2**second_level):
                for first_idx in range(starts[slot_index], starts[slot_index] + widths[slot_index]):
                    order_list.append(first_idx * 2**second_level + second)
        forward.append(tensor[order_list].T)
        backward.append(inverse[:, order_list].T)
    return (
        jnp.asarray(np.stack(forward), jnp.bfloat16),
        jnp.asarray(np.stack(backward), jnp.bfloat16),
    )


def pick(level, values):
    out = jnp.float32(values[0])
    for k in range(1, NLEV):
        out = jnp.where(level == LMIN + k, jnp.float32(values[k]), out)
    return out


def find_grid(assign_ref, me):
    def look(g, found):
        return jnp.where(assign_ref[g] == me, g, found)

    return lax.fori_loop(0, assign_ref.shape[0], look, jnp.int32(0))


def lanes():
    return lax.broadcasted_iota(jnp.int32, (8, 128), 1)


def tile(m, v):
    return pl.ds(m * SIDE + v * 8, 8)


def spread(m, v):
    return pl.ds(m * SIDE + v, 8, stride=QUADS)


def fill_speed(cs_ref, rs_ref, level, csb, speed):
    per = cs_ref.shape[1]
    for r in range(cs_ref.shape[0]):
        csb[pl.ds(r * per, per), :] = jnp.transpose(
            jnp.broadcast_to(cs_ref[pl.ds(r, 1), :], (per, per))
        )
    other = ROW_BITS - level
    inner = jnp.left_shift(jnp.int32(1), other)
    sample = jnp.bitwise_and(lanes(), inner - 1) * jnp.left_shift(jnp.int32(1), ROW_BITS - LMIN - other)
    factor = jnp.zeros((8, 128), jnp.float32)
    for k in range(rs_ref.shape[0]):
        factor = jnp.where(sample == k, rs_ref[k], factor)
    factor = factor * jnp.float32(0.5 * time_step * 2**LMIN)
    for m in range(SIDE):
        for v in range(QUADS):
            speed[tile(m, v), :] = csb[spread(m, v), :] * factor


def fill_drift(speed, level, drift):
    along = pick(level, [diffusivity * time_step * 4 ** (LMIN + k) / 2**k for k in range(NLEV)])
    for t in range(SIDE * QUADS):
        rows = pl.ds(t * 8, 8)
        one = speed[rows, :]
        drift[0, rows, :] = along - one
        drift[1, rows, :] = along + one


def advance(state, drift, level, count):
    other = ROW_BITS - level
    inner = jnp.left_shift(jnp.int32(1), other)
    refine = jnp.left_shift(jnp.int32(1), level - LMIN)
    across = [diffusivity * time_step * 4 ** (ROW_BITS - LMIN - k) / 2**k for k in range(NLEV)]
    along = [diffusivity * time_step * 4 ** (LMIN + k) / 2**k for k in range(NLEV)]
    outer = [diffusivity * time_step * 4**CLEV / 2**k for k in range(NLEV)]
    keep = [1.0 - 2.0 * across[k] - 2.0 * along[k] - 4.0 * outer[k] for k in range(NLEV)]
    coef_two = pick(level, across)
    coef_col = pick(level, outer)
    coef_own = pick(level, keep)
    shape = (SIDE, 128)
    lane = lax.broadcasted_iota(jnp.int32, shape, 1)
    place = jnp.bitwise_and(lane, inner - 1)
    at_last = place == inner - 1
    at_first = place == 0

    def one_substep(step, carry):
        now = jnp.bitwise_and(step, 1)
        later = 1 - now
        src = state.at[now]
        dst = state.at[later]

        def plane(m):
            return src[pl.ds((m % SIDE) * SIDE, SIDE), :]

        below, mid = plane(SIDE - 1), plane(0)
        for m in range(SIDE):
            above = plane(m + 1)
            rows = pl.ds(m * SIDE, SIDE)
            acc = coef_own * mid
            acc += drift[0, rows, :] * pltpu.roll(mid, 128 - inner, 1)
            acc += drift[1, rows, :] * pltpu.roll(mid, inner, 1)
            up = jnp.where(at_last, pltpu.roll(mid, inner - 1, 1), pltpu.roll(mid, 127, 1))
            down = jnp.where(at_first, pltpu.roll(mid, 129 - inner, 1), pltpu.roll(mid, 1, 1))
            acc += coef_two * (up + down)
            ahead = jnp.concatenate([mid[8:], pltpu.roll(mid[:8], 7, 0)], axis=0)
            behind = jnp.concatenate([pltpu.roll(mid[SIDE - 8 :], 1, 0), mid[: SIDE - 8]], axis=0)
            acc += coef_col * ((above + below) + (ahead + behind))
            dst[rows, :] = acc
            below, mid = mid, above
        return carry

    steps = refine * count
    lax.fori_loop(0, steps, one_substep, jnp.int32(0))
    return jnp.bitwise_and(steps, 1)


def exact_dot(values, matrix):
    high = values.astype(jnp.bfloat16)
    rest = values - high.astype(jnp.float32)
    middle = rest.astype(jnp.bfloat16)
    low = (rest - middle.astype(jnp.float32)).astype(jnp.bfloat16)
    dot = functools.partial(jnp.dot, preferred_element_type=jnp.float32)
    return dot(low, matrix) + dot(middle, matrix) + dot(high, matrix)


def pack(tiles):
    lane = lanes()
    kept = lane < SHARED
    return [jnp.where(kept, tiles[k], pltpu.roll(tiles[3], 96 - 32 * k, 1)) for k in range(3)]


def unpack(packed):
    lane = lanes()
    last = jnp.where(
        lane < 32,
        pltpu.roll(packed[0], 32, 1),
        jnp.where(lane < 64, pltpu.roll(packed[1], 64, 1), pltpu.roll(packed[2], 96, 1)),
    )
    return [packed[0], packed[1], packed[2], last]


def packed_rows(block_cols):
    return block_cols * 3 // 4 if block_cols % 32 == 0 else block_cols


def store_shared(ref, index, block_cols, group, tiles):
    if block_cols % 32 == 0:
        for k, one in enumerate(pack(tiles)):
            ref[index, pl.ds(group * 24 + k * 8, 8), :] = one
    else:
        for k, one in enumerate(tiles):
            ref[index, pl.ds(group * 32 + k * 8, 8), :] = one


def load_shared(ref, index, block_cols, group, count):
    if block_cols % 32 == 0:
        return unpack([ref[index, pl.ds(group * 24 + k * 8, 8), :] for k in range(3)])
    return [ref[index, pl.ds(group * 32 + k * 8, 8), :] for k in range(count)]


def groups_of(block_cols):
    return [(g, min(4, block_cols // 8 - 4 * g)) for g in range((block_cols + 31) // 32)]


def line_levels(bits):
    out = []
    for tier in range(1, bits + 1):
        stride = 2 ** (bits - tier)
        for entry in range(2 ** (tier - 1), 2**tier):
            out.append(((2 * (entry - 2 ** (tier - 1)) + 1) * stride, entry, stride))
    return out


def sublane_hier(x):
    sub = lax.broadcasted_iota(jnp.int32, x.shape, 0)
    fine = 0.5 * (pltpu.roll(x, 1, 0) + pltpu.roll(x, 7, 0))
    half = 0.5 * (pltpu.roll(x, 2, 0) + pltpu.roll(x, 6, 0))
    coarse = pltpu.roll(x, 4, 0)
    minus = jnp.where(
        jnp.bitwise_and(sub, 1) == 1,
        fine,
        jnp.where(jnp.bitwise_and(sub, 3) == 2, half, jnp.where(sub == 4, coarse, 0.0)),
    )
    y = x - minus
    out = y
    for entry, node in enumerate((0, 4, 2, 6, 1, 3, 5, 7)):
        if entry != node:
            out = jnp.where(sub == entry, pltpu.roll(y, (entry - node) % 8, 0), out)
    return out


def sublane_dehier(w):
    sub = lax.broadcasted_iota(jnp.int32, w.shape, 0)
    x = w
    for entry, node in enumerate((0, 4, 2, 6, 1, 3, 5, 7)):
        if entry != node:
            x = jnp.where(sub == node, pltpu.roll(w, (node - entry) % 8, 0), x)
    x = x + jnp.where(sub == 4, pltpu.roll(x, 4, 0), 0.0)
    x = x + jnp.where(jnp.bitwise_and(sub, 3) == 2, 0.5 * (pltpu.roll(x, 2, 0) + pltpu.roll(x, 6, 0)), 0.0)
    x = x + jnp.where(jnp.bitwise_and(sub, 1) == 1, 0.5 * (pltpu.roll(x, 1, 0) + pltpu.roll(x, 7, 0)), 0.0)
    return x


def column_hier(state, natural):
    def put(index, quads):
        x0, x1, x2, x3 = quads
        ahead = pltpu.roll(x0, 7, 0)
        base = index * SIDE
        natural[pl.ds(base, 8), :] = sublane_hier(x0)
        natural[pl.ds(base + 8, 8), :] = x2 - 0.5 * (x0 + ahead)
        natural[pl.ds(base + 16, 8, stride=2), :] = x1 - 0.5 * (x0 + x2)
        natural[pl.ds(base + 17, 8, stride=2), :] = x3 - 0.5 * (x2 + ahead)

    def quads(m):
        return [state[tile(m % SIDE, v), :] for v in range(QUADS)]

    put(0, quads(0))
    for node, index, stride in line_levels(CLEV):
        own, left, right = quads(node), quads(node - stride), quads(node + stride)
        put(index, [own[v] - 0.5 * (left[v] + right[v]) for v in range(QUADS)])


def column_dehier(natural, state):
    def get(index):
        base = index * SIDE
        x0 = sublane_dehier(natural[pl.ds(base, 8), :])
        ahead = pltpu.roll(x0, 7, 0)
        x2 = natural[pl.ds(base + 8, 8), :] + 0.5 * (x0 + ahead)
        x1 = natural[pl.ds(base + 16, 8, stride=2), :] + 0.5 * (x0 + x2)
        x3 = natural[pl.ds(base + 17, 8, stride=2), :] + 0.5 * (x2 + ahead)
        return [x0, x1, x2, x3]

    for v, x in enumerate(get(0)):
        state[tile(0, v), :] = x
    for node, index, stride in line_levels(CLEV):
        for v, x in enumerate(get(index)):
            left = state[tile((node - stride) % SIDE, v), :]
            right = state[tile((node + stride) % SIDE, v), :]
            state[tile(node, v), :] = x + 0.5 * (left + right)


CHUNK = 256


def first_kernel(devices, axis, start, cs, rs, levels, assign, forward, send, kept, speed, state, drift, csb):
    me = lax.axis_index(axis)
    level = levels[find_grid(assign, me)]
    total = start.shape[0]
    block_cols = total // devices
    fill_speed(cs, rs, level, csb, speed)
    fill_drift(speed, level, drift)
    for m in range(SIDE):
        for v in range(QUADS):
            state[0, tile(m, v), :] = start[spread(m, v), :]
    last = advance(state, drift, level, STEPS)
    matrix = forward[level - LMIN]
    for c in range(total // CHUNK):
        rows = pl.ds(c * CHUNK, CHUNK)
        kept[rows, :] = exact_dot(state[last, rows, :], matrix)
    for block in range(devices):
        for group, count in groups_of(block_cols):
            base = block * block_cols + group * 32
            tiles = [kept[pl.ds(base + 8 * k, 8), :] for k in range(count)]
            store_shared(send, block, block_cols, group, tiles)


def section_grids(levels, q):
    out = []
    for k in range(NLEV):
        found = jnp.int32(0)
        for j in range(NLEV):
            g = q * NLEV + j
            found = jnp.where(levels[g] == LMIN + k, g, found)
        out.append(found)
    return out


def section_weights(levels, coeffs, q):
    grids = section_grids(levels, q)
    w = [jnp.full((8, 128), coeffs[g].astype(jnp.float32)) for g in grids]
    lane = lanes()
    zero = jnp.zeros((8, 128), jnp.float32)

    def within(low, high, value):
        return jnp.where((lane >= low) & (lane < high), value, zero)

    two = [w[0], within(0, 64, w[1]), within(0, 32, w[2]), within(0, 16, w[3])]
    three = [w[1], within(64, 96, w[2]), within(64, 80, w[3])]
    four = [w[2], within(64, 96, w[3])]

    def scaled(parts):
        total = parts[0]
        for part in parts[1:]:
            total = total + part
        return [part / total for part in parts]

    return grids, scaled(two), scaled(three), scaled(four)


def combine_tile(s, two, three, four):
    x2 = (two[0] * s[0] + two[1] * s[1]) + (two[2] * s[2] + two[3] * s[3])
    d3 = three[0] * s[1] + (three[1] * pltpu.roll(s[2], 32, 1) + three[2] * pltpu.roll(s[3], 48, 1))
    d4 = four[0] * s[2] + four[1] * pltpu.roll(s[3], 32, 1)
    return x2, d3, d4


def level_tiles(x2, d3, d4, s5):
    lane = lanes()
    back3, back4 = pltpu.roll(d3, 96, 1), pltpu.roll(d4, 96, 1)
    low = lane < 64
    return [
        x2,
        jnp.where(low, x2, d3),
        jnp.where(lane < 32, x2, jnp.where(low, back3, d4)),
        jnp.where(
            lane < 16,
            x2,
            jnp.where(lane < 32, pltpu.roll(d3, 80, 1), jnp.where(low, back4, s5)),
        ),
    ]


def shared_kernel(block_cols, recv, levels, coeffs, assign, send):
    def section(q, carry):
        grids, two, three, four = section_weights(levels, coeffs, q)
        where = [assign[g] for g in grids]
        for group, count in groups_of(block_cols):
            parts = [load_shared(recv, d, block_cols, group, count) for d in where]
            made = []
            for t in range(count):
                s = [parts[k][t] for k in range(NLEV)]
                made.append(level_tiles(*combine_tile(s, two, three, four), s[3]))
            for k in range(NLEV):
                store_shared(send, where[k], block_cols, group, [made[t][k] for t in range(count)])
        return carry

    lax.fori_loop(0, recv.shape[0] // NLEV, section, jnp.int32(0))


def second_kernel(devices, axis, recv, kept, speed, levels, assign, owner, forward, backward, send, state, drift, natural):
    me = lax.axis_index(axis)
    level = levels[find_grid(assign, me)]
    total = kept.shape[0]
    block_cols = total // devices
    fill_drift(speed, level, drift)
    shared = lanes() < SHARED
    for block in range(devices):
        for group, count in groups_of(block_cols):
            tiles = load_shared(recv, block, block_cols, group, count)
            for t in range(count):
                rows = pl.ds(block * block_cols + group * 32 + 8 * t, 8)
                natural[rows, :] = jnp.where(shared, tiles[t], kept[rows, :])
    matrix = backward[level - LMIN]
    for c in range(total // CHUNK):
        rows = pl.ds(c * CHUNK, CHUNK)
        state[0, rows, :] = exact_dot(natural[rows, :], matrix)
    last = advance(state, drift, level, STEPS)
    column_hier(state.at[last], natural)
    matrix = forward[level - LMIN]
    size = max(block_cols, CHUNK)
    for c in range(total // size):
        values = exact_dot(natural[pl.ds(c * size, size), :], matrix)
        for k in range(size // block_cols):
            send[owner[c * (size // block_cols) + k], :, :] = values[k * block_cols : (k + 1) * block_cols]


def output_kernel(block_cols, recv, levels, coeffs, assign_from, assign_to, send, combined):
    low = lanes() < 64

    def pair(p, carry):
        both = [section_weights(levels, coeffs, 2 * p + k) for k in range(2)]
        for t in range(block_cols // 8):
            rows = pl.ds(t * 8, 8)
            made = []
            for grids, two, three, four in both:
                s = [recv[assign_from[g], rows, :] for g in grids]
                x2, d3, d4 = combine_tile(s, two, three, four)
                for g, one in zip(grids, level_tiles(x2, d3, d4, s[3])):
                    send[assign_to[g], rows, :] = one
                made.append((x2, d3, d4, s[3]))
            (xe, te, fe, se), (xo, to, fo, so) = made
            turned = pltpu.roll(xo, 64, 1)
            parts = [
                xe,
                jnp.where(low, pltpu.roll(te, 64, 1), fe),
                jnp.where(low, pltpu.roll(se, 64, 1), turned),
                jnp.where(low, turned, to),
                jnp.where(low, pltpu.roll(fo, 64, 1), so),
            ]
            for k, part in enumerate(parts):
                combined[rows, pl.ds(pl.multiple_of(p * 640 + k * 128, 128), 128)] = part
        return carry

    lax.fori_loop(0, recv.shape[0] // (2 * NLEV), pair, jnp.int32(0))


def last_kernel(devices, axis, recv, cs, rs, levels, assign, owner, backward, final, state, drift, natural, speed):
    me = lax.axis_index(axis)
    level = levels[find_grid(assign, me)]
    total = final.shape[0]
    block_cols = total // devices
    fill_speed(cs, rs, level, natural, speed)
    fill_drift(speed, level, drift)
    matrix = backward[level - LMIN]
    size = max(block_cols, CHUNK)
    for c in range(total // size):
        per = size // block_cols
        values = jnp.concatenate([recv[owner[c * per + k]] for k in range(per)], axis=0)
        natural[pl.ds(c * size, size), :] = exact_dot(values, matrix)
    column_dehier(natural, state.at[0])
    last = advance(state, drift, level, 1)
    for m in range(SIDE):
        for v in range(QUADS):
            final[spread(m, v), :] = state[last, tile(m, v), :]


def local(start_field, col_speed, row_speed, levels, coeffs, assign_first, assign_second, owner_of):
    forward, backward = row_tables()
    devices = lax.axis_size("grid")
    total, rows = start_field.shape[1:]
    block_cols = total // devices
    shared_rows = packed_rows(block_cols)
    sections = devices // NLEV
    section_rows = sum((2**LMIN if k == 0 else 2 ** (LMIN + k - 1)) * 2 ** (ROW_BITS - LMIN - k) for k in range(NLEV))
    cs = col_speed.reshape(-1, 128)

    def f32(*shape):
        return jax.ShapeDtypeStruct(shape, jnp.float32)

    field = (total, rows)
    state = pltpu.VMEM((2,) + field, jnp.float32)
    whole = pltpu.VMEM(field, jnp.float32)

    def exchange(blocks):
        return lax.all_to_all(blocks, "grid", split_axis=0, concat_axis=0, tiled=True)

    send, kept, speed = pl.pallas_call(
        functools.partial(first_kernel, devices, "grid"),
        name="first_cycle",
        out_shape=(f32(devices, shared_rows, rows), f32(*field), f32(*field)),
        in_specs=[VMEM, VMEM, SMEM, SMEM, SMEM, VMEM],
        out_specs=(VMEM, VMEM, VMEM),
        scratch_shapes=[state, state, whole],
    )(start_field[0], cs, row_speed, levels, assign_first, forward)
    recv = exchange(send)
    send = pl.pallas_call(
        functools.partial(shared_kernel, block_cols),
        name="shared_rows",
        out_shape=f32(devices, shared_rows, rows),
        in_specs=[VMEM, SMEM, SMEM, SMEM],
        out_specs=VMEM,
    )(recv, levels, coeffs, assign_first)
    recv = exchange(send)
    send = pl.pallas_call(
        functools.partial(second_kernel, devices, "grid"),
        name="second_cycle",
        out_shape=f32(devices, block_cols, rows),
        in_specs=[VMEM, VMEM, VMEM, SMEM, SMEM, SMEM, VMEM, VMEM],
        out_specs=VMEM,
        scratch_shapes=[state, state, whole],
    )(recv, kept, speed, levels, assign_first, owner_of, forward, backward)
    recv = exchange(send)
    send, combined = pl.pallas_call(
        functools.partial(output_kernel, block_cols),
        name="second_combined",
        out_shape=(f32(devices, block_cols, rows), f32(block_cols, sections * section_rows)),
        in_specs=[VMEM, SMEM, SMEM, SMEM, SMEM],
        out_specs=(VMEM, VMEM),
    )(recv, levels, coeffs, assign_first, assign_second)
    recv = exchange(send)
    final = pl.pallas_call(
        functools.partial(last_kernel, devices, "grid"),
        name="last_step",
        out_shape=f32(*field),
        in_specs=[VMEM, VMEM, SMEM, SMEM, SMEM, SMEM, VMEM],
        out_specs=VMEM,
        scratch_shapes=[state, state, whole, whole],
    )(recv, cs, row_speed, levels, assign_second, owner_of, backward)
    return combined, final[None]


def solution(mesh):
    placed = (
        P(("groups", "grid"), None, None),
        P(),
        P(),
        P("groups"),
        P("groups"),
        P("groups"),
        P("groups"),
        P("groups"),
    )
    return jax.shard_map(
        local,
        mesh=mesh,
        in_specs=placed,
        out_specs=(P(("groups", "grid"), None), P(("groups", "grid"), None, None)),
        check_vma=False,
    )
```

```python
import functools

import jax
import jax.numpy as jnp
import numpy as np
from jax import lax
from jax.experimental import pallas as pl
from jax.experimental.pallas import tpu as pltpu
from jax.sharding import PartitionSpec as P

LMIN = 2
NLEV = 4
CLEV = 5
STEPS = 2

time_step = 0.02
diffusivity = 0.0024

SIDE = 2**CLEV
QUADS = SIDE // 8
ROW_BITS = 2 * LMIN + NLEV - 1
SHARED = 96
PLANES = 8
SMEM = pl.BlockSpec(memory_space=pltpu.SMEM)
VMEM = pl.BlockSpec(memory_space=pltpu.VMEM)


def hier_line(line_level):
    points = 2**line_level
    matrix = np.zeros((points, points))
    matrix[0, 0] = 1.0
    for tier_rank in range(1, line_level + 1):
        stride = 2 ** (line_level - tier_rank)
        for entry_at in range(2 ** (tier_rank - 1), 2**tier_rank):
            node_at = (2 * (entry_at - 2 ** (tier_rank - 1)) + 1) * stride
            matrix[entry_at, node_at] += 1.0
            matrix[entry_at, (node_at - stride) % points] -= 0.5
            matrix[entry_at, (node_at + stride) % points] -= 0.5
    return matrix


def dehier_line(line_level):
    points = 2**line_level
    matrix = np.zeros((points, points))
    matrix[0, 0] = 1.0
    for tier_rank in range(1, line_level + 1):
        stride = 2 ** (line_level - tier_rank)
        for entry_at in range(2 ** (tier_rank - 1), 2**tier_rank):
            node_at = (2 * (entry_at - 2 ** (tier_rank - 1)) + 1) * stride
            matrix[node_at] = 0.5 * (
                matrix[(node_at - stride) % points] + matrix[(node_at + stride) % points]
            )
            matrix[node_at, entry_at] += 1.0
    return matrix


def row_tables():
    starts = [0 if k == 0 else 2 ** (LMIN + k - 1) for k in range(NLEV)]
    widths = [2**LMIN if k == 0 else 2 ** (LMIN + k - 1) for k in range(NLEV)]
    forward, backward = ([], [])
    for shift_level in range(NLEV):
        first_level = LMIN + shift_level
        second_level = ROW_BITS - first_level
        tensor = np.kron(hier_line(first_level), hier_line(second_level))
        inverse = np.kron(dehier_line(first_level), dehier_line(second_level))
        order_list = []
        for slot_index in range(shift_level + 1):
            for second in range(2**second_level):
                for first_idx in range(starts[slot_index], starts[slot_index] + widths[slot_index]):
                    order_list.append(first_idx * 2**second_level + second)
        forward.append(tensor[order_list].T)
        backward.append(inverse[:, order_list].T)
    return (
        jnp.asarray(np.stack(forward), jnp.bfloat16),
        jnp.asarray(np.stack(backward), jnp.bfloat16),
    )


def row_stencils():
    out = []
    for k in range(NLEV):
        first, second = LMIN + k, ROW_BITS - LMIN - k
        eye_one, eye_two = np.eye(2**first), np.eye(2**second)
        up_one, down_one = (np.kron(np.roll(eye_one, s, 0), eye_two) for s in (1, -1))
        up_two, down_two = (np.kron(eye_one, np.roll(eye_two, s, 0)) for s in (1, -1))
        near = 4.0 ** (first - CLEV) * (up_one + down_one) + 4.0 ** (second - CLEV) * (up_two + down_two)
        both = np.concatenate([near, up_one - down_one], axis=1)
        out.append(np.concatenate([both, both], axis=0))
    return jnp.asarray(np.stack(out), jnp.bfloat16)


def pick(level, values):
    out = jnp.float32(values[0])
    for k in range(1, NLEV):
        out = jnp.where(level == LMIN + k, jnp.float32(values[k]), out)
    return out


def find_grid(assign_ref, me):
    def look(g, found):
        return jnp.where(assign_ref[g] == me, g, found)

    return lax.fori_loop(0, assign_ref.shape[0], look, jnp.int32(0))


def lanes():
    return lax.broadcasted_iota(jnp.int32, (8, 128), 1)


def tile(m, v):
    return pl.ds(m * SIDE + v * 8, 8)


def spread(m, v):
    return pl.ds(m * SIDE + v, 8, stride=QUADS)


def fill_speed(cs_ref, rs_ref, level, csb, speed):
    per = cs_ref.shape[1]
    for r in range(cs_ref.shape[0]):
        csb[pl.ds(r * per, per), :] = jnp.transpose(
            jnp.broadcast_to(cs_ref[pl.ds(r, 1), :], (per, per))
        )
    other = ROW_BITS - level
    inner = jnp.left_shift(jnp.int32(1), other)
    sample = jnp.bitwise_and(lanes(), inner - 1) * jnp.left_shift(jnp.int32(1), ROW_BITS - LMIN - other)
    factor = jnp.zeros((8, 128), jnp.float32)
    for k in range(rs_ref.shape[0]):
        factor = jnp.where(sample == k, rs_ref[k], factor)
    factor = factor * jnp.float32(0.5 * time_step * 2**LMIN)
    for m in range(SIDE):
        for v in range(QUADS):
            speed[tile(m, v), :] = csb[spread(m, v), :] * factor


def split(values):
    high = values.astype(jnp.bfloat16)
    middle = (values - high.astype(jnp.float32)).astype(jnp.bfloat16)
    return jnp.concatenate([high, middle], axis=1)


def one_substep(source, target, speed, weights, coef_col, coef_own):
    def plane(m):
        return source[pl.ds((m % SIDE) * SIDE, SIDE), :]

    below, mid = plane(SIDE - 1), plane(0)
    for first in range(0, SIDE, PLANES):
        pieces = split(source[pl.ds(first * SIDE, PLANES * SIDE), :])
        along = jnp.dot(pieces, weights, preferred_element_type=jnp.float32)
        for m in range(first, first + PLANES):
            above = plane(m + 1)
            part = along[(m - first) * SIDE : (m - first + 1) * SIDE]
            ahead = jnp.concatenate([mid[8:], pltpu.roll(mid[:8], 7, 0)], axis=0)
            behind = jnp.concatenate([pltpu.roll(mid[SIDE - 8 :], 1, 0), mid[: SIDE - 8]], axis=0)
            around = (above + below) + (ahead + behind) + part[:, :128]
            rows = pl.ds(m * SIDE, SIDE)
            target[rows, :] = coef_own * mid + coef_col * around - speed[rows, :] * part[:, 128:]
            below, mid = mid, above


def advance(state, spare, speed, stencil, level, count):
    refine = jnp.left_shift(jnp.int32(1), level - LMIN)
    across = [diffusivity * time_step * 4 ** (ROW_BITS - LMIN - k) / 2**k for k in range(NLEV)]
    along = [diffusivity * time_step * 4 ** (LMIN + k) / 2**k for k in range(NLEV)]
    outer = [diffusivity * time_step * 4**CLEV / 2**k for k in range(NLEV)]
    keep = [1.0 - 2.0 * across[k] - 2.0 * along[k] - 4.0 * outer[k] for k in range(NLEV)]
    coef_col = pick(level, outer)
    coef_own = pick(level, keep)
    weights = stencil[level - LMIN]
    steps = refine * count

    def two(step, carry):
        one_substep(state, spare, speed, weights, coef_col, coef_own)
        one_substep(spare, state, speed, weights, coef_col, coef_own)
        return carry

    lax.fori_loop(0, jnp.right_shift(steps, 1), two, jnp.int32(0))
    if count % 2:

        @pl.when(jnp.bitwise_and(steps, 1) == 1)
        def _():
            one_substep(state, spare, speed, weights, coef_col, coef_own)
            state[...] = spare[...]


def exact_dot(values, matrix):
    high = values.astype(jnp.bfloat16)
    rest = values - high.astype(jnp.float32)
    middle = rest.astype(jnp.bfloat16)
    low = (rest - middle.astype(jnp.float32)).astype(jnp.bfloat16)
    dot = functools.partial(jnp.dot, preferred_element_type=jnp.float32)
    return dot(low, matrix) + dot(middle, matrix) + dot(high, matrix)


def pack(tiles):
    lane = lanes()
    kept = lane < SHARED
    return [jnp.where(kept, tiles[k], pltpu.roll(tiles[3], 96 - 32 * k, 1)) for k in range(3)]


def unpack(packed):
    lane = lanes()
    last = jnp.where(
        lane < 32,
        pltpu.roll(packed[0], 32, 1),
        jnp.where(lane < 64, pltpu.roll(packed[1], 64, 1), pltpu.roll(packed[2], 96, 1)),
    )
    return [packed[0], packed[1], packed[2], last]


def packed_rows(block_cols):
    return block_cols * 3 // 4 if block_cols % 32 == 0 else block_cols


def store_shared(ref, index, block_cols, group, tiles):
    if block_cols % 32 == 0:
        for k, one in enumerate(pack(tiles)):
            ref[index, pl.ds(group * 24 + k * 8, 8), :] = one
    else:
        for k, one in enumerate(tiles):
            ref[index, pl.ds(group * 32 + k * 8, 8), :] = one


def load_shared(ref, index, block_cols, group, count):
    if block_cols % 32 == 0:
        return unpack([ref[index, pl.ds(group * 24 + k * 8, 8), :] for k in range(3)])
    return [ref[index, pl.ds(group * 32 + k * 8, 8), :] for k in range(count)]


def groups_of(block_cols):
    return [(g, min(4, block_cols // 8 - 4 * g)) for g in range((block_cols + 31) // 32)]


def line_levels(bits):
    out = []
    for tier in range(1, bits + 1):
        stride = 2 ** (bits - tier)
        for entry in range(2 ** (tier - 1), 2**tier):
            out.append(((2 * (entry - 2 ** (tier - 1)) + 1) * stride, entry, stride))
    return out


def sublane_hier(x):
    sub = lax.broadcasted_iota(jnp.int32, x.shape, 0)
    fine = 0.5 * (pltpu.roll(x, 1, 0) + pltpu.roll(x, 7, 0))
    half = 0.5 * (pltpu.roll(x, 2, 0) + pltpu.roll(x, 6, 0))
    coarse = pltpu.roll(x, 4, 0)
    minus = jnp.where(
        jnp.bitwise_and(sub, 1) == 1,
        fine,
        jnp.where(jnp.bitwise_and(sub, 3) == 2, half, jnp.where(sub == 4, coarse, 0.0)),
    )
    y = x - minus
    out = y
    for entry, node in enumerate((0, 4, 2, 6, 1, 3, 5, 7)):
        if entry != node:
            out = jnp.where(sub == entry, pltpu.roll(y, (entry - node) % 8, 0), out)
    return out


def sublane_dehier(w):
    sub = lax.broadcasted_iota(jnp.int32, w.shape, 0)
    x = w
    for entry, node in enumerate((0, 4, 2, 6, 1, 3, 5, 7)):
        if entry != node:
            x = jnp.where(sub == node, pltpu.roll(w, (node - entry) % 8, 0), x)
    x = x + jnp.where(sub == 4, pltpu.roll(x, 4, 0), 0.0)
    x = x + jnp.where(jnp.bitwise_and(sub, 3) == 2, 0.5 * (pltpu.roll(x, 2, 0) + pltpu.roll(x, 6, 0)), 0.0)
    x = x + jnp.where(jnp.bitwise_and(sub, 1) == 1, 0.5 * (pltpu.roll(x, 1, 0) + pltpu.roll(x, 7, 0)), 0.0)
    return x


def column_hier(state, natural):
    def put(index, quads):
        x0, x1, x2, x3 = quads
        ahead = pltpu.roll(x0, 7, 0)
        base = index * SIDE
        natural[pl.ds(base, 8), :] = sublane_hier(x0)
        natural[pl.ds(base + 8, 8), :] = x2 - 0.5 * (x0 + ahead)
        natural[pl.ds(base + 16, 8, stride=2), :] = x1 - 0.5 * (x0 + x2)
        natural[pl.ds(base + 17, 8, stride=2), :] = x3 - 0.5 * (x2 + ahead)

    def quads(m):
        return [state[tile(m % SIDE, v), :] for v in range(QUADS)]

    put(0, quads(0))
    for node, index, stride in line_levels(CLEV):
        own, left, right = quads(node), quads(node - stride), quads(node + stride)
        put(index, [own[v] - 0.5 * (left[v] + right[v]) for v in range(QUADS)])


def column_dehier(natural, state):
    def get(index):
        base = index * SIDE
        x0 = sublane_dehier(natural[pl.ds(base, 8), :])
        ahead = pltpu.roll(x0, 7, 0)
        x2 = natural[pl.ds(base + 8, 8), :] + 0.5 * (x0 + ahead)
        x1 = natural[pl.ds(base + 16, 8, stride=2), :] + 0.5 * (x0 + x2)
        x3 = natural[pl.ds(base + 17, 8, stride=2), :] + 0.5 * (x2 + ahead)
        return [x0, x1, x2, x3]

    for v, x in enumerate(get(0)):
        state[tile(0, v), :] = x
    for node, index, stride in line_levels(CLEV):
        for v, x in enumerate(get(index)):
            left = state[tile((node - stride) % SIDE, v), :]
            right = state[tile((node + stride) % SIDE, v), :]
            state[tile(node, v), :] = x + 0.5 * (left + right)


CHUNK = 256


def first_kernel(devices, axis, start, cs, rs, levels, assign, forward, stencil, send, kept, speed, state, spare):
    me = lax.axis_index(axis)
    level = levels[find_grid(assign, me)]
    total = start.shape[0]
    block_cols = total // devices
    fill_speed(cs, rs, level, spare, speed)
    for m in range(SIDE):
        for v in range(QUADS):
            state[tile(m, v), :] = start[spread(m, v), :]
    advance(state, spare, speed, stencil, level, STEPS)
    matrix = forward[level - LMIN]
    for c in range(total // CHUNK):
        rows = pl.ds(c * CHUNK, CHUNK)
        kept[rows, :] = exact_dot(state[rows, :], matrix)
    for block in range(devices):
        for group, count in groups_of(block_cols):
            base = block * block_cols + group * 32
            tiles = [kept[pl.ds(base + 8 * k, 8), :] for k in range(count)]
            store_shared(send, block, block_cols, group, tiles)


def section_grids(levels, q):
    out = []
    for k in range(NLEV):
        found = jnp.int32(0)
        for j in range(NLEV):
            g = q * NLEV + j
            found = jnp.where(levels[g] == LMIN + k, g, found)
        out.append(found)
    return out


def section_weights(levels, coeffs, q):
    grids = section_grids(levels, q)
    w = [jnp.full((8, 128), coeffs[g].astype(jnp.float32)) for g in grids]
    lane = lanes()
    zero = jnp.zeros((8, 128), jnp.float32)

    def within(low, high, value):
        return jnp.where((lane >= low) & (lane < high), value, zero)

    two = [w[0], within(0, 64, w[1]), within(0, 32, w[2]), within(0, 16, w[3])]
    three = [w[1], within(64, 96, w[2]), within(64, 80, w[3])]
    four = [w[2], within(64, 96, w[3])]

    def scaled(parts):
        total = parts[0]
        for part in parts[1:]:
            total = total + part
        return [part / total for part in parts]

    return grids, scaled(two), scaled(three), scaled(four)


def combine_tile(s, two, three, four):
    x2 = (two[0] * s[0] + two[1] * s[1]) + (two[2] * s[2] + two[3] * s[3])
    d3 = three[0] * s[1] + (three[1] * pltpu.roll(s[2], 32, 1) + three[2] * pltpu.roll(s[3], 48, 1))
    d4 = four[0] * s[2] + four[1] * pltpu.roll(s[3], 32, 1)
    return x2, d3, d4


def level_tiles(x2, d3, d4, s5):
    lane = lanes()
    back3, back4 = pltpu.roll(d3, 96, 1), pltpu.roll(d4, 96, 1)
    low = lane < 64
    return [
        x2,
        jnp.where(low, x2, d3),
        jnp.where(lane < 32, x2, jnp.where(low, back3, d4)),
        jnp.where(
            lane < 16,
            x2,
            jnp.where(lane < 32, pltpu.roll(d3, 80, 1), jnp.where(low, back4, s5)),
        ),
    ]


def shared_kernel(block_cols, recv, levels, coeffs, assign, send):
    def section(q, carry):
        grids, two, three, four = section_weights(levels, coeffs, q)
        where = [assign[g] for g in grids]
        for group, count in groups_of(block_cols):
            parts = [load_shared(recv, d, block_cols, group, count) for d in where]
            made = []
            for t in range(count):
                s = [parts[k][t] for k in range(NLEV)]
                made.append(level_tiles(*combine_tile(s, two, three, four), s[3]))
            for k in range(NLEV):
                store_shared(send, where[k], block_cols, group, [made[t][k] for t in range(count)])
        return carry

    lax.fori_loop(0, recv.shape[0] // NLEV, section, jnp.int32(0))


def second_kernel(devices, axis, recv, kept, speed, levels, assign, owner, forward, backward, stencil, send, state, spare, natural):
    me = lax.axis_index(axis)
    level = levels[find_grid(assign, me)]
    total = kept.shape[0]
    block_cols = total // devices
    shared = lanes() < SHARED
    for block in range(devices):
        for group, count in groups_of(block_cols):
            tiles = load_shared(recv, block, block_cols, group, count)
            for t in range(count):
                rows = pl.ds(block * block_cols + group * 32 + 8 * t, 8)
                natural[rows, :] = jnp.where(shared, tiles[t], kept[rows, :])
    matrix = backward[level - LMIN]
    for c in range(total // CHUNK):
        rows = pl.ds(c * CHUNK, CHUNK)
        state[rows, :] = exact_dot(natural[rows, :], matrix)
    advance(state, spare, speed, stencil, level, STEPS)
    column_hier(state, natural)
    matrix = forward[level - LMIN]
    size = max(block_cols, CHUNK)
    for c in range(total // size):
        values = exact_dot(natural[pl.ds(c * size, size), :], matrix)
        for k in range(size // block_cols):
            send[owner[c * (size // block_cols) + k], :, :] = values[k * block_cols : (k + 1) * block_cols]


def output_kernel(block_cols, recv, levels, coeffs, assign_from, assign_to, send, combined):
    low = lanes() < 64

    def pair(p, carry):
        both = [section_weights(levels, coeffs, 2 * p + k) for k in range(2)]
        for t in range(block_cols // 8):
            rows = pl.ds(t * 8, 8)
            made = []
            for grids, two, three, four in both:
                s = [recv[assign_from[g], rows, :] for g in grids]
                x2, d3, d4 = combine_tile(s, two, three, four)
                for g, one in zip(grids, level_tiles(x2, d3, d4, s[3])):
                    send[assign_to[g], rows, :] = one
                made.append((x2, d3, d4, s[3]))
            (xe, te, fe, se), (xo, to, fo, so) = made
            turned = pltpu.roll(xo, 64, 1)
            parts = [
                xe,
                jnp.where(low, pltpu.roll(te, 64, 1), fe),
                jnp.where(low, pltpu.roll(se, 64, 1), turned),
                jnp.where(low, turned, to),
                jnp.where(low, pltpu.roll(fo, 64, 1), so),
            ]
            for k, part in enumerate(parts):
                combined[rows, pl.ds(pl.multiple_of(p * 640 + k * 128, 128), 128)] = part
        return carry

    lax.fori_loop(0, recv.shape[0] // (2 * NLEV), pair, jnp.int32(0))


def last_kernel(devices, axis, recv, cs, rs, levels, assign, owner, backward, stencil, final, state, spare, natural, speed):
    me = lax.axis_index(axis)
    level = levels[find_grid(assign, me)]
    total = final.shape[0]
    block_cols = total // devices
    fill_speed(cs, rs, level, natural, speed)
    matrix = backward[level - LMIN]
    size = max(block_cols, CHUNK)
    for c in range(total // size):
        per = size // block_cols
        values = jnp.concatenate([recv[owner[c * per + k]] for k in range(per)], axis=0)
        natural[pl.ds(c * size, size), :] = exact_dot(values, matrix)
    column_dehier(natural, state)
    advance(state, spare, speed, stencil, level, 1)
    for m in range(SIDE):
        for v in range(QUADS):
            final[spread(m, v), :] = state[tile(m, v), :]


def local(start_field, col_speed, row_speed, levels, coeffs, assign_first, assign_second, owner_of):
    forward, backward = row_tables()
    stencil = row_stencils()
    devices = lax.axis_size("grid")
    total, rows = start_field.shape[1:]
    block_cols = total // devices
    shared_rows = packed_rows(block_cols)
    sections = devices // NLEV
    section_rows = sum((2**LMIN if k == 0 else 2 ** (LMIN + k - 1)) * 2 ** (ROW_BITS - LMIN - k) for k in range(NLEV))
    cs = col_speed.reshape(-1, 128)

    def f32(*shape):
        return jax.ShapeDtypeStruct(shape, jnp.float32)

    field = (total, rows)
    whole = pltpu.VMEM(field, jnp.float32)

    def exchange(blocks):
        return lax.all_to_all(blocks, "grid", split_axis=0, concat_axis=0, tiled=True)

    send, kept, speed = pl.pallas_call(
        functools.partial(first_kernel, devices, "grid"),
        name="first_cycle",
        out_shape=(f32(devices, shared_rows, rows), f32(*field), f32(*field)),
        in_specs=[VMEM, VMEM, SMEM, SMEM, SMEM, VMEM, VMEM],
        out_specs=(VMEM, VMEM, VMEM),
        scratch_shapes=[whole, whole],
    )(start_field[0], cs, row_speed, levels, assign_first, forward, stencil)
    recv = exchange(send)
    send = pl.pallas_call(
        functools.partial(shared_kernel, block_cols),
        name="shared_rows",
        out_shape=f32(devices, shared_rows, rows),
        in_specs=[VMEM, SMEM, SMEM, SMEM],
        out_specs=VMEM,
    )(recv, levels, coeffs, assign_first)
    recv = exchange(send)
    send = pl.pallas_call(
        functools.partial(second_kernel, devices, "grid"),
        name="second_cycle",
        out_shape=f32(devices, block_cols, rows),
        in_specs=[VMEM, VMEM, VMEM, SMEM, SMEM, SMEM, VMEM, VMEM, VMEM],
        out_specs=VMEM,
        scratch_shapes=[whole, whole, whole],
    )(recv, kept, speed, levels, assign_first, owner_of, forward, backward, stencil)
    recv = exchange(send)
    send, combined = pl.pallas_call(
        functools.partial(output_kernel, block_cols),
        name="second_combined",
        out_shape=(f32(devices, block_cols, rows), f32(block_cols, sections * section_rows)),
        in_specs=[VMEM, SMEM, SMEM, SMEM, SMEM],
        out_specs=(VMEM, VMEM),
    )(recv, levels, coeffs, assign_first, assign_second)
    recv = exchange(send)
    final = pl.pallas_call(
        functools.partial(last_kernel, devices, "grid"),
        name="last_step",
        out_shape=f32(*field),
        in_specs=[VMEM, VMEM, SMEM, SMEM, SMEM, SMEM, VMEM, VMEM],
        out_specs=VMEM,
        scratch_shapes=[whole, whole, whole, whole],
    )(recv, cs, row_speed, levels, assign_second, owner_of, backward, stencil)
    return combined, final[None]


def solution(mesh):
    placed = (
        P(("groups", "grid"), None, None),
        P(),
        P(),
        P("groups"),
        P("groups"),
        P("groups"),
        P("groups"),
        P("groups"),
    )
    return jax.shard_map(
        local,
        mesh=mesh,
        in_specs=placed,
        out_specs=(P(("groups", "grid"), None), P(("groups", "grid"), None, None)),
        check_vma=False,
    )
```

```python
import functools

import jax
import jax.numpy as jnp
import numpy as np
from jax import lax
from jax.experimental import pallas as pl
from jax.experimental.pallas import tpu as pltpu
from jax.sharding import PartitionSpec as P

LMIN = 2
NLEV = 4
CLEV = 5
STEPS = 2

time_step = 0.02
diffusivity = 0.0024

SIDE = 2**CLEV
QUADS = SIDE // 8
ROW_BITS = 2 * LMIN + NLEV - 1
SHARED = 96
PLANES = 8
PARAMS = pltpu.CompilerParams(vmem_limit_bytes=12 * 2**20)
SMEM = pl.BlockSpec(memory_space=pltpu.SMEM)
VMEM = pl.BlockSpec(memory_space=pltpu.VMEM)
HBM = pl.BlockSpec(memory_space=pltpu.HBM)


def hier_line(line_level):
    points = 2**line_level
    matrix = np.zeros((points, points))
    matrix[0, 0] = 1.0
    for tier_rank in range(1, line_level + 1):
        stride = 2 ** (line_level - tier_rank)
        for entry_at in range(2 ** (tier_rank - 1), 2**tier_rank):
            node_at = (2 * (entry_at - 2 ** (tier_rank - 1)) + 1) * stride
            matrix[entry_at, node_at] += 1.0
            matrix[entry_at, (node_at - stride) % points] -= 0.5
            matrix[entry_at, (node_at + stride) % points] -= 0.5
    return matrix


def dehier_line(line_level):
    points = 2**line_level
    matrix = np.zeros((points, points))
    matrix[0, 0] = 1.0
    for tier_rank in range(1, line_level + 1):
        stride = 2 ** (line_level - tier_rank)
        for entry_at in range(2 ** (tier_rank - 1), 2**tier_rank):
            node_at = (2 * (entry_at - 2 ** (tier_rank - 1)) + 1) * stride
            matrix[node_at] = 0.5 * (
                matrix[(node_at - stride) % points] + matrix[(node_at + stride) % points]
            )
            matrix[node_at, entry_at] += 1.0
    return matrix


def row_tables():
    starts = [0 if k == 0 else 2 ** (LMIN + k - 1) for k in range(NLEV)]
    widths = [2**LMIN if k == 0 else 2 ** (LMIN + k - 1) for k in range(NLEV)]
    forward, backward = ([], [])
    for shift_level in range(NLEV):
        first_level = LMIN + shift_level
        second_level = ROW_BITS - first_level
        tensor = np.kron(hier_line(first_level), hier_line(second_level))
        inverse = np.kron(dehier_line(first_level), dehier_line(second_level))
        order_list = []
        for slot_index in range(shift_level + 1):
            for second in range(2**second_level):
                for first_idx in range(starts[slot_index], starts[slot_index] + widths[slot_index]):
                    order_list.append(first_idx * 2**second_level + second)
        forward.append(tensor[order_list].T)
        backward.append(inverse[:, order_list].T)
    return (
        jnp.asarray(np.stack(forward), jnp.bfloat16),
        jnp.asarray(np.stack(backward), jnp.bfloat16),
    )


def row_stencils():
    out = []
    for k in range(NLEV):
        first, second = LMIN + k, ROW_BITS - LMIN - k
        eye_one, eye_two = np.eye(2**first), np.eye(2**second)
        up_one, down_one = (np.kron(np.roll(eye_one, s, 0), eye_two) for s in (1, -1))
        up_two, down_two = (np.kron(eye_one, np.roll(eye_two, s, 0)) for s in (1, -1))
        near = 4.0 ** (first - CLEV) * (up_one + down_one) + 4.0 ** (second - CLEV) * (up_two + down_two)
        both = np.concatenate([near, up_one - down_one], axis=1)
        out.append(np.concatenate([both, both], axis=0))
    return jnp.asarray(np.stack(out), jnp.bfloat16)


def pick(level, values):
    out = jnp.float32(values[0])
    for k in range(1, NLEV):
        out = jnp.where(level == LMIN + k, jnp.float32(values[k]), out)
    return out


def find_grid(assign_ref, me):
    def look(g, found):
        return jnp.where(assign_ref[g] == me, g, found)

    return lax.fori_loop(0, assign_ref.shape[0], look, jnp.int32(0))


def lanes():
    return lax.broadcasted_iota(jnp.int32, (8, 128), 1)


def tile(m, v):
    return pl.ds(m * SIDE + v * 8, 8)


def spread(m, v):
    return pl.ds(m * SIDE + v, 8, stride=QUADS)


def fill_speed(cs_ref, rs_ref, level, csb, speed):
    per = cs_ref.shape[1]
    for r in range(cs_ref.shape[0]):
        csb[pl.ds(r * per, per), :] = jnp.transpose(
            jnp.broadcast_to(cs_ref[pl.ds(r, 1), :], (per, per))
        )
    other = ROW_BITS - level
    inner = jnp.left_shift(jnp.int32(1), other)
    sample = jnp.bitwise_and(lanes(), inner - 1) * jnp.left_shift(jnp.int32(1), ROW_BITS - LMIN - other)
    factor = jnp.zeros((8, 128), jnp.float32)
    for k in range(rs_ref.shape[0]):
        factor = jnp.where(sample == k, rs_ref[k], factor)
    factor = factor * jnp.float32(0.5 * time_step * 2**LMIN)
    for m in range(SIDE):
        for v in range(QUADS):
            speed[tile(m, v), :] = csb[spread(m, v), :] * factor


def split(values):
    high = values.astype(jnp.bfloat16)
    middle = (values - high.astype(jnp.float32)).astype(jnp.bfloat16)
    return jnp.concatenate([high, middle], axis=1)


def one_substep(source, target, speed, weights, coef_col, coef_own):
    def plane(m):
        return source[pl.ds((m % SIDE) * SIDE, SIDE), :]

    below, mid = plane(SIDE - 1), plane(0)
    for first in range(0, SIDE, PLANES):
        pieces = split(source[pl.ds(first * SIDE, PLANES * SIDE), :])
        along = jnp.dot(pieces, weights, preferred_element_type=jnp.float32)
        for m in range(first, first + PLANES):
            above = plane(m + 1)
            part = along[(m - first) * SIDE : (m - first + 1) * SIDE]
            ahead = jnp.concatenate([mid[8:], pltpu.roll(mid[:8], 7, 0)], axis=0)
            behind = jnp.concatenate([pltpu.roll(mid[SIDE - 8 :], 1, 0), mid[: SIDE - 8]], axis=0)
            around = (above + below) + (ahead + behind) + part[:, :128]
            rows = pl.ds(m * SIDE, SIDE)
            target[rows, :] = coef_own * mid + coef_col * around - speed[rows, :] * part[:, 128:]
            below, mid = mid, above


def advance(state, spare, speed, stencil, level, count):
    refine = jnp.left_shift(jnp.int32(1), level - LMIN)
    across = [diffusivity * time_step * 4 ** (ROW_BITS - LMIN - k) / 2**k for k in range(NLEV)]
    along = [diffusivity * time_step * 4 ** (LMIN + k) / 2**k for k in range(NLEV)]
    outer = [diffusivity * time_step * 4**CLEV / 2**k for k in range(NLEV)]
    keep = [1.0 - 2.0 * across[k] - 2.0 * along[k] - 4.0 * outer[k] for k in range(NLEV)]
    coef_col = pick(level, outer)
    coef_own = pick(level, keep)
    weights = stencil[...]
    steps = refine * count

    def two(step, carry):
        one_substep(state, spare, speed, weights, coef_col, coef_own)
        one_substep(spare, state, speed, weights, coef_col, coef_own)
        return carry

    lax.fori_loop(0, jnp.right_shift(steps, 1), two, jnp.int32(0))
    if count % 2:

        @pl.when(jnp.bitwise_and(steps, 1) == 1)
        def _():
            one_substep(state, spare, speed, weights, coef_col, coef_own)
            state[...] = spare[...]


def in_hbm(x):
    return pltpu.with_memory_space_constraint(x, pltpu.HBM)


def exact_dot(values, matrix):
    high = values.astype(jnp.bfloat16)
    rest = values - high.astype(jnp.float32)
    middle = rest.astype(jnp.bfloat16)
    low = (rest - middle.astype(jnp.float32)).astype(jnp.bfloat16)
    dot = functools.partial(jnp.dot, preferred_element_type=jnp.float32)
    return dot(low, matrix) + dot(middle, matrix) + dot(high, matrix)


def pack(tiles):
    lane = lanes()
    kept = lane < SHARED
    return [jnp.where(kept, tiles[k], pltpu.roll(tiles[3], 96 - 32 * k, 1)) for k in range(3)]


def unpack(packed):
    lane = lanes()
    last = jnp.where(
        lane < 32,
        pltpu.roll(packed[0], 32, 1),
        jnp.where(lane < 64, pltpu.roll(packed[1], 64, 1), pltpu.roll(packed[2], 96, 1)),
    )
    return [packed[0], packed[1], packed[2], last]


def packed_rows(block_cols):
    return block_cols * 3 // 4 if block_cols % 32 == 0 else block_cols


def store_shared(ref, index, block_cols, group, tiles):
    if block_cols % 32 == 0:
        for k, one in enumerate(pack(tiles)):
            ref[index, pl.ds(group * 24 + k * 8, 8), :] = one
    else:
        for k, one in enumerate(tiles):
            ref[index, pl.ds(group * 32 + k * 8, 8), :] = one


def load_shared(ref, index, block_cols, group, count):
    if block_cols % 32 == 0:
        return unpack([ref[index, pl.ds(group * 24 + k * 8, 8), :] for k in range(3)])
    return [ref[index, pl.ds(group * 32 + k * 8, 8), :] for k in range(count)]


def groups_of(block_cols):
    return [(g, min(4, block_cols // 8 - 4 * g)) for g in range((block_cols + 31) // 32)]


def line_levels(bits):
    out = []
    for tier in range(1, bits + 1):
        stride = 2 ** (bits - tier)
        for entry in range(2 ** (tier - 1), 2**tier):
            out.append(((2 * (entry - 2 ** (tier - 1)) + 1) * stride, entry, stride))
    return out


def sublane_hier(x):
    sub = lax.broadcasted_iota(jnp.int32, x.shape, 0)
    fine = 0.5 * (pltpu.roll(x, 1, 0) + pltpu.roll(x, 7, 0))
    half = 0.5 * (pltpu.roll(x, 2, 0) + pltpu.roll(x, 6, 0))
    coarse = pltpu.roll(x, 4, 0)
    minus = jnp.where(
        jnp.bitwise_and(sub, 1) == 1,
        fine,
        jnp.where(jnp.bitwise_and(sub, 3) == 2, half, jnp.where(sub == 4, coarse, 0.0)),
    )
    y = x - minus
    out = y
    for entry, node in enumerate((0, 4, 2, 6, 1, 3, 5, 7)):
        if entry != node:
            out = jnp.where(sub == entry, pltpu.roll(y, (entry - node) % 8, 0), out)
    return out


def sublane_dehier(w):
    sub = lax.broadcasted_iota(jnp.int32, w.shape, 0)
    x = w
    for entry, node in enumerate((0, 4, 2, 6, 1, 3, 5, 7)):
        if entry != node:
            x = jnp.where(sub == node, pltpu.roll(w, (node - entry) % 8, 0), x)
    x = x + jnp.where(sub == 4, pltpu.roll(x, 4, 0), 0.0)
    x = x + jnp.where(jnp.bitwise_and(sub, 3) == 2, 0.5 * (pltpu.roll(x, 2, 0) + pltpu.roll(x, 6, 0)), 0.0)
    x = x + jnp.where(jnp.bitwise_and(sub, 1) == 1, 0.5 * (pltpu.roll(x, 1, 0) + pltpu.roll(x, 7, 0)), 0.0)
    return x


def column_hier(state, natural):
    def put(index, quads):
        x0, x1, x2, x3 = quads
        ahead = pltpu.roll(x0, 7, 0)
        base = index * SIDE
        natural[pl.ds(base, 8), :] = sublane_hier(x0)
        natural[pl.ds(base + 8, 8), :] = x2 - 0.5 * (x0 + ahead)
        natural[pl.ds(base + 16, 8, stride=2), :] = x1 - 0.5 * (x0 + x2)
        natural[pl.ds(base + 17, 8, stride=2), :] = x3 - 0.5 * (x2 + ahead)

    def quads(m):
        return [state[tile(m % SIDE, v), :] for v in range(QUADS)]

    put(0, quads(0))
    for node, index, stride in line_levels(CLEV):
        own, left, right = quads(node), quads(node - stride), quads(node + stride)
        put(index, [own[v] - 0.5 * (left[v] + right[v]) for v in range(QUADS)])


def column_dehier(natural, state):
    def get(index):
        base = index * SIDE
        x0 = sublane_dehier(natural[pl.ds(base, 8), :])
        ahead = pltpu.roll(x0, 7, 0)
        x2 = natural[pl.ds(base + 8, 8), :] + 0.5 * (x0 + ahead)
        x1 = natural[pl.ds(base + 16, 8, stride=2), :] + 0.5 * (x0 + x2)
        x3 = natural[pl.ds(base + 17, 8, stride=2), :] + 0.5 * (x2 + ahead)
        return [x0, x1, x2, x3]

    for v, x in enumerate(get(0)):
        state[tile(0, v), :] = x
    for node, index, stride in line_levels(CLEV):
        for v, x in enumerate(get(index)):
            left = state[tile((node - stride) % SIDE, v), :]
            right = state[tile((node + stride) % SIDE, v), :]
            state[tile(node, v), :] = x + 0.5 * (left + right)


CHUNK = 256


def first_kernel(
    devices,
    axis,
    start_hbm,
    cs_hbm,
    rs_hbm,
    levels_hbm,
    assign_hbm,
    forward_hbm,
    stencil_hbm,
    send,
    kept,
    speed,
    state,
    spare,
    start,
    cs,
    forward,
    stencil,
    rs,
    levels,
    assign,
    sems,
):
    def copy(k, source, target):
        one = pltpu.make_async_copy(source, target, sems.at[k])
        one.start()
        return one

    ints = [copy(0, levels_hbm, levels), copy(1, assign_hbm, assign)]
    speeds = [copy(2, rs_hbm, rs), copy(3, cs_hbm, cs)]
    values = copy(4, start_hbm, start)
    for one in ints:
        one.wait()
    me = lax.axis_index(axis)
    level = levels[find_grid(assign, me)]
    tables = [
        copy(5, stencil_hbm.at[level - LMIN], stencil),
        copy(6, forward_hbm.at[level - LMIN], forward),
    ]
    total = start.shape[0]
    block_cols = total // devices
    for one in speeds:
        one.wait()
    fill_speed(cs, rs, level, spare, speed)
    values.wait()
    for m in range(SIDE):
        for v in range(QUADS):
            state[tile(m, v), :] = start[spread(m, v), :]
    for one in tables:
        one.wait()
    advance(state, spare, speed, stencil, level, STEPS)
    matrix = forward[...]
    for c in range(total // CHUNK):
        rows = pl.ds(c * CHUNK, CHUNK)
        kept[rows, :] = exact_dot(state[rows, :], matrix)
    for block in range(devices):
        for group, count in groups_of(block_cols):
            base = block * block_cols + group * 32
            tiles = [kept[pl.ds(base + 8 * k, 8), :] for k in range(count)]
            store_shared(send, block, block_cols, group, tiles)


def section_grids(levels, q):
    out = []
    for k in range(NLEV):
        found = jnp.int32(0)
        for j in range(NLEV):
            g = q * NLEV + j
            found = jnp.where(levels[g] == LMIN + k, g, found)
        out.append(found)
    return out


def section_weights(levels, coeffs, q):
    grids = section_grids(levels, q)
    w = [jnp.full((8, 128), coeffs[g].astype(jnp.float32)) for g in grids]
    lane = lanes()
    zero = jnp.zeros((8, 128), jnp.float32)

    def within(low, high, value):
        return jnp.where((lane >= low) & (lane < high), value, zero)

    two = [w[0], within(0, 64, w[1]), within(0, 32, w[2]), within(0, 16, w[3])]
    three = [w[1], within(64, 96, w[2]), within(64, 80, w[3])]
    four = [w[2], within(64, 96, w[3])]

    def scaled(parts):
        total = parts[0]
        for part in parts[1:]:
            total = total + part
        return [part / total for part in parts]

    return grids, scaled(two), scaled(three), scaled(four)


def combine_tile(s, two, three, four):
    x2 = (two[0] * s[0] + two[1] * s[1]) + (two[2] * s[2] + two[3] * s[3])
    d3 = three[0] * s[1] + (three[1] * pltpu.roll(s[2], 32, 1) + three[2] * pltpu.roll(s[3], 48, 1))
    d4 = four[0] * s[2] + four[1] * pltpu.roll(s[3], 32, 1)
    return x2, d3, d4


def level_tiles(x2, d3, d4, s5):
    lane = lanes()
    back3, back4 = pltpu.roll(d3, 96, 1), pltpu.roll(d4, 96, 1)
    low = lane < 64
    return [
        x2,
        jnp.where(low, x2, d3),
        jnp.where(lane < 32, x2, jnp.where(low, back3, d4)),
        jnp.where(
            lane < 16,
            x2,
            jnp.where(lane < 32, pltpu.roll(d3, 80, 1), jnp.where(low, back4, s5)),
        ),
    ]


def shared_kernel(block_cols, recv, levels, coeffs, assign, send):
    def section(q, carry):
        grids, two, three, four = section_weights(levels, coeffs, q)
        where = [assign[g] for g in grids]
        for group, count in groups_of(block_cols):
            parts = [load_shared(recv, d, block_cols, group, count) for d in where]
            made = []
            for t in range(count):
                s = [parts[k][t] for k in range(NLEV)]
                made.append(level_tiles(*combine_tile(s, two, three, four), s[3]))
            for k in range(NLEV):
                store_shared(send, where[k], block_cols, group, [made[t][k] for t in range(count)])
        return carry

    lax.fori_loop(0, recv.shape[0] // NLEV, section, jnp.int32(0))


def second_kernel(devices, axis, recv, kept, speed, levels, assign, owner_hbm, forward, backward, stencil, send, state, spare, natural, owner, sem):
    owners = pltpu.make_async_copy(owner_hbm, owner, sem)
    owners.start()
    me = lax.axis_index(axis)
    level = levels[find_grid(assign, me)]
    total = kept.shape[0]
    block_cols = total // devices
    shared = lanes() < SHARED
    for block in range(devices):
        for group, count in groups_of(block_cols):
            tiles = load_shared(recv, block, block_cols, group, count)
            for t in range(count):
                rows = pl.ds(block * block_cols + group * 32 + 8 * t, 8)
                natural[rows, :] = jnp.where(shared, tiles[t], kept[rows, :])
    matrix = backward[level - LMIN]
    for c in range(total // CHUNK):
        rows = pl.ds(c * CHUNK, CHUNK)
        state[rows, :] = exact_dot(natural[rows, :], matrix)
    advance(state, spare, speed, stencil.at[level - LMIN], level, STEPS)
    column_hier(state, natural)
    owners.wait()
    matrix = forward[level - LMIN]
    size = max(block_cols, CHUNK)
    for c in range(total // size):
        values = exact_dot(natural[pl.ds(c * size, size), :], matrix)
        for k in range(size // block_cols):
            send[owner[c * (size // block_cols) + k], :, :] = values[k * block_cols : (k + 1) * block_cols]


def output_kernel(block_cols, recv, levels, coeffs, assign_from, assign_to, send, combined):
    low = lanes() < 64

    def pair(p, carry):
        both = [section_weights(levels, coeffs, 2 * p + k) for k in range(2)]
        for t in range(block_cols // 8):
            rows = pl.ds(t * 8, 8)
            made = []
            for grids, two, three, four in both:
                s = [recv[assign_from[g], rows, :] for g in grids]
                x2, d3, d4 = combine_tile(s, two, three, four)
                for g, one in zip(grids, level_tiles(x2, d3, d4, s[3])):
                    send[assign_to[g], rows, :] = one
                made.append((x2, d3, d4, s[3]))
            (xe, te, fe, se), (xo, to, fo, so) = made
            turned = pltpu.roll(xo, 64, 1)
            parts = [
                xe,
                jnp.where(low, pltpu.roll(te, 64, 1), fe),
                jnp.where(low, pltpu.roll(se, 64, 1), turned),
                jnp.where(low, turned, to),
                jnp.where(low, pltpu.roll(fo, 64, 1), so),
            ]
            for k, part in enumerate(parts):
                combined[rows, pl.ds(pl.multiple_of(p * 640 + k * 128, 128), 128)] = part
        return carry

    lax.fori_loop(0, recv.shape[0] // (2 * NLEV), pair, jnp.int32(0))


def last_kernel(devices, axis, recv, cs, rs, levels, assign, owner, backward, stencil, final, state, spare, natural, speed):
    me = lax.axis_index(axis)
    level = levels[find_grid(assign, me)]
    total = final.shape[0]
    block_cols = total // devices
    fill_speed(cs, rs, level, natural, speed)
    matrix = backward[level - LMIN]
    size = max(block_cols, CHUNK)
    for c in range(total // size):
        per = size // block_cols
        values = jnp.concatenate([recv[owner[c * per + k]] for k in range(per)], axis=0)
        natural[pl.ds(c * size, size), :] = exact_dot(values, matrix)
    column_dehier(natural, state)
    advance(state, spare, speed, stencil.at[level - LMIN], level, 1)
    for m in range(SIDE):
        for v in range(QUADS):
            final[spread(m, v), :] = state[tile(m, v), :]


def local(start_field, col_speed, row_speed, levels, coeffs, assign_first, assign_second, owner_of):
    forward, backward = row_tables()
    stencil = row_stencils()
    devices = lax.axis_size("grid")
    total, rows = start_field.shape[1:]
    block_cols = total // devices
    shared_rows = packed_rows(block_cols)
    sections = devices // NLEV
    section_rows = sum((2**LMIN if k == 0 else 2 ** (LMIN + k - 1)) * 2 ** (ROW_BITS - LMIN - k) for k in range(NLEV))
    cs = col_speed.reshape(-1, 128)

    def f32(*shape):
        return jax.ShapeDtypeStruct(shape, jnp.float32)

    field = (total, rows)
    whole = pltpu.VMEM(field, jnp.float32)

    def exchange(blocks):
        return lax.all_to_all(blocks, "grid", split_axis=0, concat_axis=0, tiled=True)

    first_args = (start_field[0], cs, row_speed, levels, assign_first, forward, stencil)
    send, kept, speed = pl.pallas_call(
        functools.partial(first_kernel, devices, "grid"),
        name="first_cycle",
        compiler_params=PARAMS,
        out_shape=(f32(devices, shared_rows, rows), f32(*field), f32(*field)),
        in_specs=[HBM] * 7,
        out_specs=(VMEM, VMEM, VMEM),
        scratch_shapes=[
            whole,
            whole,
            whole,
            pltpu.VMEM(cs.shape, jnp.float32),
            pltpu.VMEM(forward.shape[1:], jnp.bfloat16),
            pltpu.VMEM(stencil.shape[1:], jnp.bfloat16),
            pltpu.SMEM(row_speed.shape, jnp.float32),
            pltpu.SMEM(levels.shape, jnp.int32),
            pltpu.SMEM(levels.shape, jnp.int32),
            pltpu.SemaphoreType.DMA((7,)),
        ],
    )(*(in_hbm(x) for x in first_args))
    recv = exchange(send)
    send = pl.pallas_call(
        functools.partial(shared_kernel, block_cols),
        name="shared_rows",
        compiler_params=PARAMS,
        out_shape=f32(devices, shared_rows, rows),
        in_specs=[VMEM, SMEM, SMEM, SMEM],
        out_specs=VMEM,
    )(recv, levels, coeffs, assign_first)
    recv = exchange(send)
    send = pl.pallas_call(
        functools.partial(second_kernel, devices, "grid"),
        name="second_cycle",
        compiler_params=PARAMS,
        out_shape=f32(devices, block_cols, rows),
        in_specs=[VMEM, VMEM, VMEM, SMEM, SMEM, HBM, VMEM, VMEM, VMEM],
        out_specs=VMEM,
        scratch_shapes=[whole, whole, whole, pltpu.SMEM(owner_of.shape, jnp.int32), pltpu.SemaphoreType.DMA],
    )(recv, kept, speed, levels, assign_first, in_hbm(owner_of), forward, backward, stencil)
    recv = exchange(send)
    send, combined = pl.pallas_call(
        functools.partial(output_kernel, block_cols),
        name="second_combined",
        compiler_params=PARAMS,
        out_shape=(f32(devices, block_cols, rows), f32(block_cols, sections * section_rows)),
        in_specs=[VMEM, SMEM, SMEM, SMEM, SMEM],
        out_specs=(VMEM, VMEM),
    )(recv, levels, coeffs, assign_first, assign_second)
    recv = exchange(send)
    final = pl.pallas_call(
        functools.partial(last_kernel, devices, "grid"),
        name="last_step",
        compiler_params=PARAMS,
        out_shape=f32(*field),
        in_specs=[VMEM, VMEM, SMEM, SMEM, SMEM, SMEM, VMEM, VMEM],
        out_specs=VMEM,
        scratch_shapes=[whole, whole, whole, whole],
    )(recv, cs, row_speed, levels, assign_second, owner_of, backward, stencil)
    return combined, final[None]


def solution(mesh):
    placed = (
        P(("groups", "grid"), None, None),
        P(),
        P(),
        P("groups"),
        P("groups"),
        P("groups"),
        P("groups"),
        P("groups"),
    )
    return jax.shard_map(
        local,
        mesh=mesh,
        in_specs=placed,
        out_specs=(P(("groups", "grid"), None), P(("groups", "grid"), None, None)),
        check_vma=False,
    )
```
